32 devices in a mesh: fsdp: 8 (over z, core), tp: 4 (over y, x).
Axes of the slice: x: 2, y: 2, z: 4, core: 2. Of those that a mesh axis runs over, the one named last changes fastest.
Arguments:
- tokens: bfloat16 [80, 16384], P('tp', 'fsdp'), may hold values from -6 to 6
- gate_weight: bfloat16 [16384, 28672], P('fsdp', 'tp'), may hold values from -0.046875 to 0.046875
- up_weight: bfloat16 [16384, 28672], P('fsdp', 'tp'), may hold values from -0.046875 to 0.046875
- down_weight: bfloat16 [28672, 16384], P('tp', 'fsdp'), may hold values from -0.03125 to 0.03125
Outputs:
- layer_out: bfloat16 [80, 16384], P('tp', 'fsdp')
The draws below stay inside these ranges and needn't reach their ends.
All inputs are finite; a program needn't handle non-finite values.
Results may differ from the reference program's by a relative error of at most 0.019.
Values may be sent and summed in bfloat16 or wider, within the bound.
A program may use at most 128 MiB of HBM per device.

```python
import jax
import jax.numpy as jnp

D = 16384
FF = 28672
TOKENS = 80


def levels(rng, dims, split, least, high):
    factor_of, own = 1.0, jax.random.fold_in(rng, 6)
    for dim, blocks in split:
        draws = jnp.exp(jax.random.uniform(jax.random.fold_in(own, dim), (blocks,), jnp.float32, least / len(split), high / len(split)))
        factor_of = factor_of * jnp.repeat(draws, dims[dim] // blocks).reshape([-1 if axis == dim else 1 for axis in range(len(dims))])
    return factor_of


def normal_values(stream_key, extent, deviation, limit, pieces=(), dtype=jnp.bfloat16):
    result = deviation * jax.random.normal(stream_key, extent, jnp.float32)
    if pieces:
        result = result * levels(stream_key, extent, pieces, -0.22, 0.18)
    return jnp.clip(result, -limit, limit).astype(dtype)


def setup_inputs(seed: int = 0) -> dict:
    key_of = jax.random.split(jax.random.key(seed), 5)
    return {
        "tokens": normal_values(key_of[0], (TOKENS, D), 1.0, 6.0, ((0, 4), (1, 8))),
        "gate_weight": normal_values(key_of[1], (D, FF), D ** -0.5, 0.046875, ((0, 8), (1, 4))),
        "up_weight": normal_values(key_of[2], (D, FF), D ** -0.5, 0.046875, ((0, 8), (1, 4))),
        "down_weight": normal_values(key_of[3], (FF, D), FF ** -0.5, 0.03125, ((0, 4), (1, 8))),
    }


def reference(tokens, gate_weight, up_weight, down_weight):
    gate_sum = jnp.dot(tokens, gate_weight, preferred_element_type=jnp.float32)
    up_sum = jnp.dot(tokens, up_weight, preferred_element_type=jnp.float32)
    hidden = (jax.nn.silu(gate_sum) * up_sum).astype(jnp.bfloat16)
    return jnp.dot(hidden, down_weight, preferred_element_type=jnp.float32).astype(jnp.bfloat16)
```

```python
import functools

import jax
import jax.numpy as jnp
from jax import lax
from jax.experimental import pallas as pl
from jax.experimental.pallas import tpu as pltpu
from jax.sharding import PartitionSpec as P

MESH = pl.DeviceIdType.MESH
F32, BF16 = jnp.float32, jnp.bfloat16
LANES, PACK = 128, 16
VMEM_LIMIT = 66_000_000


def placing(shape, rows, padded, parts, along):
    wide = lax.broadcasted_iota(jnp.int32, shape, along)
    tight = lax.broadcasted_iota(jnp.int32, shape, 1 - along)
    hit = jnp.zeros(shape, F32)
    for part in range(parts):
        here = (tight >= part * rows) & (tight < (part + 1) * rows)
        hit = jnp.where(here & (wide - part * padded == tight - part * rows), 1.0, hit)
    return hit.astype(BF16)


def kernel(F, T, R, tok, gate, up, down, out, gath, seg, wbuf, dn, part, pin, red, zin, hall, acc, obuf, oin,
           wsem, dsem, tsend, trecv, psend, precv, zsend, zrecv, hsend, hrecv, fsend, frecv, osend, orecv):
    Z = F // 2
    RP, DL = tok.shape
    K, W = hall.shape[0], F * LANES
    half = Z * LANES
    f, t = lax.axis_index("fsdp"), lax.axis_index("tp")
    z, c = f // 2, f % 2
    partner = z * 2 + (1 - c)
    place = c * Z + z

    def chip(o):
        return lax.rem(z + o, Z) * 2 + c

    def peer(o):
        return lax.rem(t + o, T)

    def remote(src, dst, send, recv, where):
        return pltpu.make_async_remote_copy(src_ref=src, dst_ref=dst, send_sem=send, recv_sem=recv,
                                            device_id=where, device_id_type=MESH)

    def weights(k):
        slot = lax.rem(k, 2)
        cols = pl.ds(pl.multiple_of(k * W, W), W)
        return [pltpu.make_async_copy(w.at[:, cols], wbuf.at[slot, i], wsem.at[slot, i]) for i, w in enumerate((gate, up))]

    def downs(k):
        return pltpu.make_async_copy(down.at[pl.ds(pl.multiple_of(k * W, W), W), :], dn.at[k], dsem.at[k])

    def pair(k):
        return remote(part.at[k, 1 - c], pin.at[k], psend.at[k], precv.at[k], {"fsdp": partner})

    def across(k, o):
        return remote(red.at[k, lax.rem(z + o, Z)], zin.at[k, o - 1], zsend.at[k, o - 1], zrecv.at[k, o - 1], {"fsdp": chip(o)})

    def spread(k, o):
        return remote(hall.at[k, place], hall.at[k, place], hsend.at[k, o - 1], hrecv.at[k, o - 1], {"fsdp": chip(o)})

    def forward(k):
        mine = pl.ds(c * Z, Z)
        return remote(hall.at[k, mine], hall.at[k, mine], fsend.at[k], frecv.at[k], {"fsdp": partner})

    def tokens(o):
        return remote(tok, gath.at[t], tsend.at[o - 1], trecv.at[o - 1], {"tp": peer(o)})

    def result(o):
        return remote(obuf.at[peer(o)], oin.at[o - 1], osend.at[o - 1], orecv.at[o - 1], {"tp": peer(o)})

    for k in range(min(2, K)):
        for copy in weights(k):
            copy.start()

    barrier = pltpu.get_barrier_semaphore()
    pl.semaphore_signal(barrier, inc=1, device_id={"fsdp": partner}, device_id_type=MESH)
    for o in range(1, Z):
        pl.semaphore_signal(barrier, inc=1, device_id={"fsdp": chip(o)}, device_id_type=MESH)
    for o in range(1, T):
        pl.semaphore_signal(barrier, inc=1, device_id={"tp": peer(o)}, device_id_type=MESH)
    pl.semaphore_wait(barrier, 1 + (Z - 1) + (T - 1))

    for o in range(1, T):
        tokens(o).start()
    gath[t] = tok[...]
    acc[...] = jnp.zeros_like(acc)
    for o in range(1, T):
        tokens(o).wait()
    seg[...] = jnp.dot(placing((T * R, T * RP), R, RP, T, 1), gath[...].reshape(T * RP, DL),
                       preferred_element_type=F32).astype(BF16)

    def step(k, carry):
        @pl.when(k < K)
        def _():
            slot = lax.rem(k, 2)
            for copy in weights(k):
                copy.wait()
            for i in range(2):
                for h in range(2):
                    part[k, h, i] = jnp.dot(seg[...], wbuf[slot, i, :, h * half:(h + 1) * half],
                                            preferred_element_type=F32).astype(BF16)
            pair(k).start()

            @pl.when(k + 2 < K)
            def _():
                for copy in weights(k + 2):
                    copy.start()

            @pl.when(k == max(K - 2, 0))
            def _():
                for j in range(K):
                    downs(j).start()

        @pl.when((k >= 1) & (k - 1 < K))
        def _():
            j = k - 1
            pair(j).wait_recv()
            for i in range(2):
                both = part[j, c, i].astype(F32) + pin[j, i].astype(F32)
                for zz in range(Z):
                    red[j, zz, i] = both[:, zz * LANES:(zz + 1) * LANES].astype(BF16)
            for o in range(1, Z):
                across(j, o).start()

        @pl.when((k >= 3) & (k - 3 < K))
        def _():
            j = k - 3
            sums = [red[j, z, i].astype(F32) for i in range(2)]
            for o in range(1, Z):
                across(j, o).wait_recv()
                sums = [sums[i] + zin[j, o - 1, i].astype(F32) for i in range(2)]
            g, u = sums
            hall[j, place] = (g / (1.0 + jnp.exp(-g)) * u).astype(BF16)
            for o in range(1, Z):
                spread(j, o).start()

        @pl.when((k >= 5) & (k - 5 < K))
        def _():
            j = k - 5
            for o in range(1, Z):
                spread(j, o).wait_recv()
            forward(j).start()

        @pl.when((k >= 6) & (k - 6 < K))
        def _():
            j = k - 6
            downs(j).wait()
            forward(j).wait_recv()
            hidden = jnp.concatenate([hall[j, p] for p in range(F)], axis=1)
            span = 512 if DL % 512 == 0 else LANES
            for n in range(0, DL, span):
                acc[:, n:n + span] += jnp.dot(hidden, dn[j, :, n:n + span], preferred_element_type=F32)

        return carry

    lax.fori_loop(0, K + 6, step, 0)

    obuf[...] = jnp.dot(placing((T * RP, T * R), R, RP, T, 0), acc[...].astype(BF16),
                        preferred_element_type=F32).astype(BF16).reshape(T, RP, DL)
    for o in range(1, T):
        result(o).start()

    def drain(k, carry):
        pair(k).wait_send()
        forward(k).wait_send()
        for o in range(1, Z):
            across(k, o).wait_send()
            spread(k, o).wait_send()
        return carry

    lax.fori_loop(0, K, drain, 0)
    total = obuf[t].astype(F32)
    for o in range(1, T):
        result(o).wait()
        total = total + oin[o - 1].astype(F32)
    out[...] = total.astype(BF16)[:R]


def fused(F, T, tokens, gate_weight, up_weight, down_weight):
    R, DL = tokens.shape
    FL = gate_weight.shape[1]
    RP = -(-R // PACK) * PACK
    W, Z, M = F * LANES, F // 2, T * R
    K = FL // W
    padded = jnp.pad(tokens, ((0, RP - R), (0, 0)))
    dma = pltpu.SemaphoreType.DMA
    vmem = pltpu.VMEM
    flops = 2 * M * DL * FL * 3
    return pl.pallas_call(
        functools.partial(kernel, F, T, R),
        out_shape=jax.ShapeDtypeStruct((R, DL), BF16),
        in_specs=[pl.BlockSpec(memory_space=pltpu.VMEM)] + [pl.BlockSpec(memory_space=pl.ANY)] * 3,
        out_specs=pl.BlockSpec(memory_space=pltpu.VMEM),
        scratch_shapes=[
            vmem((T, RP, DL), BF16), vmem((M, DL), BF16),
            vmem((2, 2, DL, W), BF16), vmem((K, W, DL), BF16),
            vmem((K, 2, 2, M, Z * LANES), BF16), vmem((K, 2, M, Z * LANES), BF16),
            vmem((K, Z, 2, M, LANES), BF16), vmem((K, Z - 1, 2, M, LANES), BF16),
            vmem((K, F, M, LANES), BF16), vmem((M, DL), F32),
            vmem((T, RP, DL), BF16), vmem((T - 1, RP, DL), BF16),
            dma((2, 2)), dma((K,)), dma((T - 1,)), dma((T - 1,)), dma((K,)), dma((K,)),
            dma((K, Z - 1)), dma((K, Z - 1)), dma((K, Z - 1)), dma((K, Z - 1)),
            dma((K,)), dma((K,)), dma((T - 1,)), dma((T - 1,)),
        ],
        compiler_params=pltpu.CompilerParams(collective_id=0, has_side_effects=True, vmem_limit_bytes=VMEM_LIMIT),
        cost_estimate=pl.CostEstimate(flops=flops, bytes_accessed=6 * DL * FL, transcendentals=0),
        name="swiglu_block",
    )(padded, gate_weight, up_weight, down_weight)


def per_device(F, T, tokens, gate_weight, up_weight, down_weight):
    DL, FL = gate_weight.shape
    held = 2 * (FL * DL + 4 * DL * F * LANES)
    if F % 4 == 0 and T > 1 and FL % (F * LANES) == 0 and DL % LANES == 0 and held < VMEM_LIMIT - 2**23:
        return fused(F, T, tokens, gate_weight, up_weight, down_weight)
    segment = lax.all_gather(tokens, "tp", axis=0, tiled=True)
    gate_part = jnp.dot(segment, gate_weight, preferred_element_type=F32)
    up_part = jnp.dot(segment, up_weight, preferred_element_type=F32)
    partials = jnp.stack([gate_part, up_part])
    summed = lax.psum_scatter(partials, "fsdp", scatter_dimension=2, tiled=True)
    hidden = (jax.nn.silu(summed[0]) * summed[1]).astype(BF16)
    outputs = jnp.dot(lax.all_gather(hidden, "fsdp", axis=1, tiled=True), down_weight, preferred_element_type=F32)
    return lax.psum_scatter(outputs.astype(BF16), "tp", scatter_dimension=0, tiled=True)


def solution(mesh):
    placed = (P("tp", "fsdp"), P("fsdp", "tp"), P("fsdp", "tp"), P("tp", "fsdp"))
    return jax.shard_map(
        functools.partial(per_device, mesh.shape["fsdp"], mesh.shape["tp"]),
        mesh=mesh, in_specs=placed, out_specs=P("tp", "fsdp"), check_vma=False,
    )
```
